8 devices in a mesh: ep: 8 (over z, y, x, core).
Axes of the slice: x: 2, y: 2, z: 1, core: 2. Of those that a mesh axis runs over, the one named last changes fastest.
Arguments:
- x_tokens: bfloat16 [16384, 768], P('ep')
- grad_out: bfloat16 [16384, 768], P('ep')
- w_router: bfloat16 [768, 16], replicated
- expert_ids: int32 [16384], P('ep')
- w_in: bfloat16 [16, 768, 3072], P('ep')
- w_out: bfloat16 [16, 3072, 768], P('ep')
Outputs:
- output 1: bfloat16 [16384, 768], P('ep')
- output 2: bfloat16 [16384, 768], P('ep')
- output 3: float32 [], replicated
- output 4: float32 [], replicated
- output 5: float32 [768, 16], replicated
- output 6: float32 [16, 768, 3072], P('ep')
- output 7: float32 [16, 3072, 768], P('ep')
All inputs are finite; a program needn't handle non-finite values.
Results may differ from the reference program's by a relative error of at most 0.0163146.
Values are sent between devices in bfloat16 or wider.
A program may use at most 1 GiB of HBM per device.

```python
import math
import jax
import jax.numpy as jnp
from jax import lax

GROUP = 8
TOKENS_DEV = 2048
D = 768
FF = 3072
EXPERTS = 16
CAP = 160
AUX_WEIGHT = 0.01
Z_WEIGHT = 0.001


def draw_ids(key):
    total_tokens = GROUP * TOKENS_DEV
    key_a, key_b, key_c, key_d = jax.random.split(key, 4)
    first_pick = jax.random.randint(key_a, (GROUP, TOKENS_DEV), 0, EXPERTS)
    second_pick = jax.random.randint(key_b, (GROUP, TOKENS_DEV), 0, EXPERTS)
    favored = jax.random.randint(key_c, (GROUP, 1), 0, EXPERTS)
    coin_flip = jax.random.randint(key_d, (GROUP, TOKENS_DEV), 0, 8)
    skewed = jnp.where(coin_flip < 5, jnp.minimum(first_pick, second_pick), first_pick)
    choice = jnp.where(coin_flip < 3, favored, skewed).reshape(total_tokens)
    position = jnp.arange(total_tokens)
    return jnp.where(position < EXPERTS, position, choice).astype(jnp.int32)


def setup_inputs(seed: int = 0) -> dict:
    total_tokens = GROUP * TOKENS_DEV
    key_list = jax.random.split(jax.random.key(seed), 7)
    device_scale = jax.random.uniform(key_list[6], (GROUP, 1, 1), jnp.float32, 0.5, 1.5)
    x_tokens = (jax.random.normal(key_list[0], (GROUP, TOKENS_DEV, D), jnp.float32) * device_scale).reshape(total_tokens, D)
    out_scale = 0.04 / (total_tokens * math.sqrt(D))
    grad_out = jax.random.normal(key_list[1], (total_tokens, D), jnp.float32) * out_scale
    w_router = jax.random.normal(key_list[2], (D, EXPERTS), jnp.float32) / math.sqrt(D)
    w_in = jax.random.normal(key_list[4], (EXPERTS, D, FF), jnp.float32) / math.sqrt(D)
    w_out = jax.random.normal(key_list[5], (EXPERTS, FF, D), jnp.float32) / math.sqrt(FF)
    return {
        "x_tokens": x_tokens.astype(jnp.bfloat16),
        "grad_out": grad_out.astype(jnp.bfloat16),
        "w_router": w_router.astype(jnp.bfloat16),
        "expert_ids": draw_ids(key_list[3]),
        "w_in": w_in.astype(jnp.bfloat16),
        "w_out": w_out.astype(jnp.bfloat16),
    }


def gather_rows(table_rows, row_index):
    return jnp.take(table_rows, row_index, axis=0, mode="fill", fill_value=0)


def dispatch_plan(device_ids):
    onehot = (device_ids[:, None] == jnp.arange(EXPERTS, dtype=jnp.int32)[None, :]).astype(jnp.int32)
    position = jnp.sum(jnp.cumsum(onehot, axis=0) * onehot, axis=1) - 1
    slot_of = jnp.where(position < CAP, device_ids * CAP + position, EXPERTS * CAP)
    token_of = jnp.full((EXPERTS * CAP,), TOKENS_DEV, jnp.int32).at[slot_of].set(
        jnp.arange(TOKENS_DEV, dtype=jnp.int32), mode="drop")
    return slot_of, token_of


def to_experts(slot_rows):
    return slot_rows.reshape(GROUP, EXPERTS, CAP, D).transpose(1, 0, 2, 3).reshape(EXPERTS, GROUP * CAP, D)


def to_devices(slot_rows):
    return slot_rows.reshape(EXPERTS, GROUP, CAP, D).transpose(1, 0, 2, 3).reshape(GROUP, EXPERTS * CAP, D)


def expert_pass(operands):
    slot_x, slot_dy, weight_in, weight_out = operands
    hidden = jnp.maximum(jnp.dot(slot_x, weight_in, preferred_element_type=jnp.float32), 0.0).astype(jnp.bfloat16)
    slot_y = jnp.dot(hidden, weight_out, preferred_element_type=jnp.float32).astype(jnp.bfloat16)
    grad_wout = jnp.dot(hidden.T, slot_dy, preferred_element_type=jnp.float32)
    grad_hidden = jnp.where(hidden > 0, jnp.dot(slot_dy, weight_out.T, preferred_element_type=jnp.float32), 0.0).astype(jnp.bfloat16)
    grad_win = jnp.dot(slot_x.T, grad_hidden, preferred_element_type=jnp.float32)
    slot_dx = jnp.dot(grad_hidden, weight_in.T, preferred_element_type=jnp.float32).astype(jnp.bfloat16)
    return slot_y, slot_dx, grad_win, grad_wout


def reference(x_tokens, grad_out, w_router, expert_ids, w_in, w_out):
    total_tokens = GROUP * TOKENS_DEV
    logits = jnp.dot(x_tokens, w_router, preferred_element_type=jnp.float32)
    log_norm = jax.nn.logsumexp(logits, axis=1)
    router_prob = jnp.exp(logits - log_norm[:, None])
    chosen = (expert_ids[:, None] == jnp.arange(EXPERTS, dtype=jnp.int32)[None, :]).astype(jnp.float32)
    gate_val = jnp.sum(chosen * router_prob, axis=1)
    route_frac = jnp.sum(chosen, axis=0) / total_tokens
    aux_loss = EXPERTS * jnp.sum(route_frac * jnp.mean(router_prob, axis=0))
    z_loss = jnp.mean(log_norm * log_norm)

    slot_of, token_of = jax.vmap(dispatch_plan)(expert_ids.reshape(GROUP, TOKENS_DEV))
    grad_y = (gate_val[:, None] * grad_out.astype(jnp.float32)).astype(jnp.bfloat16)
    send_x = jax.vmap(gather_rows)(x_tokens.reshape(GROUP, TOKENS_DEV, D), token_of)
    send_dy = jax.vmap(gather_rows)(grad_y.reshape(GROUP, TOKENS_DEV, D), token_of)
    slot_y, slot_dx, grad_w_in, grad_w_out = lax.map(expert_pass, (to_experts(send_x), to_experts(send_dy), w_in, w_out))
    y_tok = jax.vmap(gather_rows)(to_devices(slot_y), slot_of).reshape(total_tokens, D)
    grad_expert = jax.vmap(gather_rows)(to_devices(slot_dx), slot_of).reshape(total_tokens, D)

    y_out = (gate_val[:, None] * y_tok.astype(jnp.float32)).astype(jnp.bfloat16)
    main_term = jnp.sum(y_out.astype(jnp.float32) * grad_out.astype(jnp.float32))
    objective = main_term + AUX_WEIGHT * aux_loss + Z_WEIGHT * z_loss

    grad_gate = jnp.sum(grad_out.astype(jnp.float32) * y_tok.astype(jnp.float32), axis=1)
    mix_frac = jnp.sum(router_prob * route_frac[None, :], axis=1, keepdims=True)
    grad_logits = ((grad_gate * gate_val)[:, None] * (chosen - router_prob)
                   + (AUX_WEIGHT * EXPERTS / total_tokens) * router_prob * (route_frac[None, :] - mix_frac)
                   + (2.0 * Z_WEIGHT / total_tokens) * log_norm[:, None] * router_prob)
    grad_logit_b = grad_logits.astype(jnp.bfloat16)
    router_part = jnp.dot(grad_logit_b, w_router.T, preferred_element_type=jnp.float32)
    grad_x = (grad_expert.astype(jnp.float32) + router_part).astype(jnp.bfloat16)
    grad_router = jnp.dot(x_tokens.T, grad_logit_b, preferred_element_type=jnp.float32)
    return y_out, grad_x, objective, main_term, grad_router, grad_w_in, grad_w_out
```

```python
import functools

import jax
import jax.numpy as jnp
from jax import lax
from jax.experimental import pallas as pl
from jax.experimental.pallas import tpu as pltpu
from jax.sharding import PartitionSpec as P

AUX_WEIGHT = 0.01
Z_WEIGHT = 0.001
MESH = pl.DeviceIdType.MESH
GRP = 8
TILE = 256
STRIDE = 512
F32, BF16, I32 = jnp.float32, jnp.bfloat16, jnp.int32
NT = (((1,), (1,)), ((), ()))
TN = (((0,), (0,)), ((), ()))
ANY = pl.BlockSpec(memory_space=pl.ANY)


def iota(shape, dim):
    return lax.broadcasted_iota(I32, shape, dim)


def plan_kernel(group, experts, own, capacity, ids_ref, slot_ref, meta_ref, sbuf, rbuf, send_sem, recv_sem):
    tokens = ids_ref.shape[1]
    me = lax.axis_index("ep")
    barrier = pltpu.get_barrier_semaphore()
    for k in range(1, group):
        pl.semaphore_signal(barrier, inc=1, device_id=(lax.rem(me + k, group),), device_id_type=MESH)

    onehot = ids_ref[...] == iota((experts, tokens), 0)
    ohb = onehot.astype(F32).astype(BF16)
    counts = lax.dot_general(jnp.ones((8, tokens), BF16), ohb, NT, preferred_element_type=F32)
    sbuf[...] = jnp.zeros_like(sbuf)
    sbuf[:, :experts] = counts
    rbuf[pl.ds(me, 1)] = jnp.zeros((1, 8, 128), F32)
    rbuf[pl.ds(me, 1), :, :experts] = counts[None]

    chunks = tokens // 128
    stacked = jnp.concatenate([ohb[:, c * 128:(c + 1) * 128] for c in range(chunks)], axis=0)
    upper = (iota((128, 128), 0) <= iota((128, 128), 1)).astype(F32).astype(BF16)
    prefix = jnp.dot(stacked, upper, preferred_element_type=F32)

    pl.semaphore_wait(barrier, group - 1)
    copies = []
    for k in range(1, group):
        copy = pltpu.make_async_remote_copy(
            src_ref=sbuf, dst_ref=rbuf.at[me], send_sem=send_sem.at[k - 1], recv_sem=recv_sem.at[k - 1],
            device_id=(lax.rem(me + k, group),), device_id_type=MESH)
        copy.start()
        copies.append(copy)

    carry = jnp.zeros((experts, 1), F32)
    places = []
    for c in range(chunks):
        part = prefix[c * experts:(c + 1) * experts]
        places.append(part + carry)
        carry = carry + part[:, 127:128]
    groups_col = ((jnp.minimum(carry.astype(I32), capacity) + (GRP - 1)) >> 3).astype(F32)
    ahead = (iota((experts, experts), 0) > iota((experts, experts), 1)) & (
        iota((experts, experts), 0) // own == iota((experts, experts), 1) // own)
    base = jnp.dot(ahead.astype(F32).astype(BF16), jnp.broadcast_to(groups_col, (experts, 128)).astype(BF16),
                   preferred_element_type=F32).astype(I32) * GRP
    base = base + jnp.bitwise_xor(iota((experts, 128), 0) // own, me) * STRIDE
    for c in range(chunks):
        mask = onehot[:, c * 128:(c + 1) * 128]
        place = jnp.sum(jnp.where(mask, places[c], 0.0), axis=0, keepdims=True).astype(I32) - 1
        start = jnp.sum(jnp.where(mask, base, 0), axis=0, keepdims=True)
        slot_ref[:, c * 128:(c + 1) * 128] = jnp.where(place < capacity, start + place, group * STRIDE)

    for copy in copies:
        copy.wait()

    row, lane = iota((group, 128), 0), iota((group, 128), 1)
    raw = jnp.concatenate([rbuf[s, 0:1, :] for s in range(group)], axis=0).astype(I32)
    groups = (jnp.minimum(raw, capacity) + (GRP - 1)) >> 3
    spread = jnp.zeros((group, 128), I32)
    for l in range(own):
        column = jnp.sum(jnp.where(lane == me * own + l, groups, 0), axis=1, keepdims=True)
        spread = spread + jnp.where(lax.rem(lane, own) == l, column, 0)
    held = jnp.sum(jnp.where(jnp.bitwise_xor(lane // own, me) == row, spread, 0), axis=0, keepdims=True)
    meta_ref[...] = jnp.concatenate([
        held, jnp.sum(raw, axis=0, keepdims=True), jnp.zeros((6, 128), I32)], axis=0)


def plan(ids_row, group, experts, own, capacity):
    tokens = ids_row.shape[1]
    return pl.pallas_call(
        functools.partial(plan_kernel, group, experts, own, capacity),
        out_shape=(jax.ShapeDtypeStruct((1, tokens), I32), jax.ShapeDtypeStruct((8, 128), I32)),
        in_specs=[pl.BlockSpec(memory_space=pltpu.VMEM)],
        out_specs=[pl.BlockSpec(memory_space=pltpu.VMEM)] * 2,
        scratch_shapes=[pltpu.VMEM((8, 128), F32), pltpu.VMEM((group, 8, 128), F32),
                        pltpu.SemaphoreType.DMA((group - 1,)), pltpu.SemaphoreType.DMA((group - 1,))],
        compiler_params=pltpu.CompilerParams(collective_id=0, has_side_effects=True),
        name="plan",
    )(ids_row)


def pack_kernel(group, slot_ref, rows_ref, *refs):
    outs, (held, sem) = refs[:group], refs[group:]
    size, tokens = held.shape[1], slot_ref.shape[1]
    copies = []
    for k in range(group):
        pick = (slot_ref[...] - k * STRIDE == iota((size, tokens), 0)).astype(F32).astype(BF16)
        held[k] = jnp.dot(pick, rows_ref[...], preferred_element_type=F32).astype(BF16)
        copy = pltpu.make_async_copy(held.at[k], outs[k], sem.at[k])
        copy.start()
        copies.append(copy)
    for copy in copies:
        copy.wait()


def pack(slot_row, rows, group, size):
    tokens, dim = rows.shape
    return pl.pallas_call(
        functools.partial(pack_kernel, group),
        out_shape=[jax.ShapeDtypeStruct((size, dim), BF16)] * group,
        in_specs=[pl.BlockSpec(memory_space=pltpu.VMEM)] * 2,
        out_specs=[ANY] * group,
        scratch_shapes=[pltpu.VMEM((group, size, dim), BF16), pltpu.SemaphoreType.DMA((group,))],
        cost_estimate=pl.CostEstimate(flops=2 * group * size * tokens * dim, bytes_accessed=4 * tokens * dim, transcendentals=0),
        name="pack",
    )(slot_row, rows)


def route_kernel(experts, x_ref, g_ref, w_ref, ids_ref, slot_ref, dy_ref, info_ref, sums_ref):
    rows = x_ref.shape[0]
    logits = jnp.dot(x_ref[...], w_ref[...], preferred_element_type=F32)
    top = jnp.max(logits, axis=1, keepdims=True)
    lse = top + jnp.log(jnp.sum(jnp.exp(logits - top), axis=1, keepdims=True))
    prob = jnp.exp(logits - lse)
    chosen = ids_ref[...] == iota((rows, experts), 1)
    gate = jnp.sum(jnp.where(chosen, prob, 0.0), axis=1, keepdims=True)
    dy_ref[...] = (gate * g_ref[...].astype(F32)).astype(BF16)
    info_ref[:, :experts] = prob
    info_ref[:, experts:experts + 1] = lse
    info_ref[:, experts + 1:experts + 2] = gate
    info_ref[:, experts + 2:experts + 3] = ids_ref[...].astype(F32)
    info_ref[:, experts + 3:experts + 4] = slot_ref[...].astype(F32)

    @pl.when(pl.program_id(0) == 0)
    def _():
        sums_ref[...] = jnp.zeros_like(sums_ref)
    sums_ref[0:1, :experts] += jnp.sum(prob, axis=0, keepdims=True)
    sums_ref[0:1, experts:experts + 1] += jnp.sum(lse * lse, axis=0, keepdims=True)


def route(x, grad_out, w_router, ids_col, slot_col, block=512):
    tokens, dim = x.shape
    experts = w_router.shape[1]
    return pl.pallas_call(
        functools.partial(route_kernel, experts), grid=(tokens // block,),
        out_shape=(jax.ShapeDtypeStruct((tokens, dim), BF16), jax.ShapeDtypeStruct((tokens, 128), F32),
                   jax.ShapeDtypeStruct((8, dim), F32)),
        in_specs=[pl.BlockSpec((block, dim), lambda i: (i, 0)), pl.BlockSpec((block, dim), lambda i: (i, 0)),
                  pl.BlockSpec((dim, experts), lambda i: (0, 0)), pl.BlockSpec((block, 1), lambda i: (i, 0)),
                  pl.BlockSpec((block, 1), lambda i: (i, 0))],
        out_specs=[pl.BlockSpec((block, dim), lambda i: (i, 0)), pl.BlockSpec((block, 128), lambda i: (i, 0)),
                   pl.BlockSpec((8, dim), lambda i: (0, 0))],
        cost_estimate=pl.CostEstimate(flops=2 * tokens * dim * 128, bytes_accessed=6 * tokens * dim, transcendentals=0),
        name="route",
    )(x, grad_out, w_router, ids_col, slot_col)


def run_table(held, own):
    group = held.shape[0] // own
    sizes = held.reshape(group, own)
    inside = jnp.cumsum(sizes, axis=1) - sizes
    dense = jnp.cumsum(sizes, axis=0) - sizes
    total = jnp.broadcast_to(jnp.sum(sizes, axis=0)[None], sizes.shape)
    return jnp.stack([sizes, inside, dense, total]).astype(I32).reshape(-1)


class Runs:
    def __init__(self, ref, group, own):
        self.ref, self.group, self.own = ref, group, own

    def get(self, kind, k, e):
        return self.ref[(kind * self.group + k) * self.own + e]

    def size(self, k, e):
        return self.get(0, k, e)

    def inside(self, k, e):
        return self.get(1, k, e)

    def dense(self, k, e):
        return self.get(2, k, e)

    def rows(self, e):
        return self.get(3, 0, e) * GRP

    def tiles(self, e):
        return (self.rows(e) + (TILE - 1)) // TILE


def each_run(runs, e, act, make):
    for k in range(runs.group):
        size = runs.size(k, e)

        @pl.when(size > 0)
        def _():
            getattr(make(k, size), act)()


def fill(runs, e, parts, dense, sem, act):
    def make(k, size):
        return pltpu.make_async_copy(parts[k].at[pl.ds(runs.inside(k, e), size)],
                                     dense.at[e, pl.ds(runs.dense(k, e), size)], sem.at[e, k])
    each_run(runs, e, act, make)


def drain(runs, e, dense, parts, sem, act):
    def make(k, size):
        return pltpu.make_async_copy(dense.at[e, pl.ds(runs.dense(k, e), size)],
                                     parts[k].at[pl.ds(runs.inside(k, e), size)], sem.at[e, k])
    each_run(runs, e, act, make)


def blank(runs, zeros, parts, sem, act):
    for k in range(runs.group):
        used = sum(runs.size(k, e) for e in range(runs.own))
        left = parts[k].shape[0] - used

        @pl.when(left > 0)
        def _():
            getattr(pltpu.make_async_copy(zeros.at[pl.ds(0, left)], parts[k].at[pl.ds(used, left)], sem.at[k]), act)()


def ffn_frame(runs, ins, outs, dense_in, dense_out, zeros, in_sem, out_sem, blank_sem):
    e, step = pl.program_id(0), pl.program_id(1)
    last = pl.num_programs(1) - 1

    @pl.when((e == 0) & (step == 0))
    def _():
        zeros[...] = jnp.zeros_like(zeros)
        for i in range(runs.own):
            fill(runs, i, ins, dense_in, in_sem, "start")

    for i in range(runs.own):
        @pl.when((e == i) & (step == 0))
        def _():
            fill(runs, i, ins, dense_in, in_sem, "wait")

    def after():
        for i in range(runs.own):
            @pl.when((e == i) & (step == last))
            def _():
                drain(runs, i, dense_out, outs, out_sem, "start")

        @pl.when((e == runs.own - 1) & (step == last))
        def _():
            blank(runs, zeros, outs, blank_sem, "start")
            for i in range(runs.own):
                drain(runs, i, dense_out, outs, out_sem, "wait")
            blank(runs, zeros, outs, blank_sem, "wait")
    return after


def tile_rows(i):
    return pl.ds(pl.multiple_of(i * TILE, TILE), TILE)


def tile_groups(i):
    return pl.ds(i * (TILE // GRP), TILE // GRP)


def accumulate(step, last, acc, at, part, store):
    @pl.when(step == 0)
    def _():
        acc[at] = part

    @pl.when((step > 0) & (step < last))
    def _():
        acc[at] += part

    @pl.when(step == last)
    def _():
        store((acc[at] + part).astype(BF16))


def ffn_kernel(group, backward, table_ref, *refs):
    ins, refs = refs[:group], refs[group:]
    if backward:
        h_ref, refs = refs[0], refs[1:]
    win_ref, wout_ref = refs[:2]
    outs, refs = refs[2:2 + group], refs[2 + group:]
    mid_ref, clean_ref, acc, dense_in, dense_out, zeros, in_sem, out_sem, blank_sem = refs
    own = dense_in.shape[0]
    runs = Runs(table_ref, group, own)
    e, step, last = pl.program_id(0), pl.program_id(1), pl.num_programs(1) - 1
    dim = win_ref.shape[1]
    after = ffn_frame(runs, ins, outs, dense_in, dense_out, zeros, in_sem, out_sem, blank_sem)
    rows = runs.rows(e)

    def body(i, _):
        at = tile_rows(i)

        @pl.when(step == 0)
        def _():
            fresh = dense_in[e, tile_groups(i)].reshape(TILE, dim)
            clean_ref[at] = jnp.where(i * TILE + iota((TILE, dim), 0) < rows, fresh, jnp.zeros_like(fresh))

        if backward:
            full = lax.dot_general(clean_ref[at], wout_ref[0], NT, preferred_element_type=F32)
            mid = jnp.where(h_ref[at].astype(F32) > 0.0, full, 0.0).astype(BF16)
            part = lax.dot_general(mid, win_ref[0], NT, preferred_element_type=F32)
        else:
            mid = jnp.maximum(jnp.dot(clean_ref[at], win_ref[0], preferred_element_type=F32), 0.0).astype(BF16)
            part = jnp.dot(mid, wout_ref[0], preferred_element_type=F32)
        mid_ref[at] = mid

        def store(value):
            dense_out[e, tile_groups(i)] = value.reshape(TILE // GRP, GRP, dim)
        accumulate(step, last, acc, at, part, store)
        return 0

    lax.fori_loop(0, runs.tiles(e), body, 0)
    after()


def ffn(table, parts, hidden, w_in, w_out, capacity, block=1024):
    group = len(parts)
    own, dim, ff = w_in.shape
    held = group * capacity
    size = parts[0].shape[0] // GRP
    grouped = [p.reshape(size, GRP, dim) for p in parts]
    extra = [] if hidden is None else [hidden]
    result = pl.pallas_call(
        functools.partial(ffn_kernel, group, hidden is not None),
        out_shape=[jax.ShapeDtypeStruct((size, GRP, dim), BF16)] * group + [
            jax.ShapeDtypeStruct((own * held, ff), BF16), jax.ShapeDtypeStruct((own * held, dim), BF16)],
        grid_spec=pltpu.PrefetchScalarGridSpec(
            num_scalar_prefetch=1, grid=(own, ff // block),
            in_specs=[ANY] * group + [pl.BlockSpec((held, block), lambda e, f, t: (e, f))] * len(extra) + [
                pl.BlockSpec((1, dim, block), lambda e, f, t: (e, 0, f)),
                pl.BlockSpec((1, block, dim), lambda e, f, t: (e, f, 0))],
            out_specs=[ANY] * group + [pl.BlockSpec((held, block), lambda e, f, t: (e, f)),
                                       pl.BlockSpec((held, dim), lambda e, f, t: (e, 0))],
            scratch_shapes=[pltpu.VMEM((held, dim), F32),
                            pltpu.VMEM((own, held // GRP, GRP, dim), BF16), pltpu.VMEM((own, held // GRP, GRP, dim), BF16),
                            pltpu.VMEM((size, GRP, dim), BF16),
                            pltpu.SemaphoreType.DMA((own, group)), pltpu.SemaphoreType.DMA((own, group)),
                            pltpu.SemaphoreType.DMA((group,))]),
        cost_estimate=pl.CostEstimate(flops=3 * own * held * dim * ff, bytes_accessed=40 << 20, transcendentals=0),
        name="ffn_forward" if hidden is None else "ffn_backward",
    )(table, *grouped, *extra, w_in, w_out)
    return [r.reshape(size * GRP, dim) for r in result[:group]], result[group], result[group + 1]


def ffn_weights(table, x, dy, hidden, grad_hidden, own, group, block=512):
    dim, ff = x.shape[1], hidden.shape[1]
    rows = x.shape[0] // own

    def kernel(table_ref, *refs):
        r = Runs(table_ref, group, own)
        return weights_body(r, *refs)

    return pl.pallas_call(
        kernel,
        out_shape=(jax.ShapeDtypeStruct((own, dim, ff), F32), jax.ShapeDtypeStruct((own, ff, dim), F32)),
        grid_spec=pltpu.PrefetchScalarGridSpec(
            num_scalar_prefetch=1, grid=(own, ff // block),
            in_specs=[pl.BlockSpec((rows, dim), lambda e, f, t: (e, 0)),
                      pl.BlockSpec((rows, dim), lambda e, f, t: (e, 0)),
                      pl.BlockSpec((rows, block), lambda e, f, t: (e, f)),
                      pl.BlockSpec((rows, block), lambda e, f, t: (e, f))],
            out_specs=[pl.BlockSpec((1, dim, block), lambda e, f, t: (e, 0, f)),
                       pl.BlockSpec((1, block, dim), lambda e, f, t: (e, f, 0))]),
        cost_estimate=pl.CostEstimate(flops=3 * own * rows * dim * ff, bytes_accessed=60 << 20, transcendentals=0),
        name="ffn_weights",
    )(table, x, dy, hidden, grad_hidden)


def weights_body(runs, x_ref, dy_ref, h_ref, dh_ref, gin_ref, gout_ref):
    gin_ref[...] = jnp.zeros_like(gin_ref)
    gout_ref[...] = jnp.zeros_like(gout_ref)

    def body(i, _):
        at = tile_rows(i)
        gin_ref[0] += lax.dot_general(x_ref[at], dh_ref[at], TN, preferred_element_type=F32)
        gout_ref[0] += lax.dot_general(h_ref[at], dy_ref[at], TN, preferred_element_type=F32)
        return 0

    lax.fori_loop(0, runs.tiles(pl.program_id(0)), body, 0)


def gather_parts(parts, held, sem):
    size = parts[0].shape[0]

    @pl.when(pl.program_id(0) == 0)
    def _():
        copies = [pltpu.make_async_copy(part, held.at[pl.ds(k * size, size)], sem.at[k]) for k, part in enumerate(parts)]
        for copy in copies:
            copy.start()
        for copy in copies:
            copy.wait()


def unpick(info, lane_at, rows, size, group):
    code = info[:, lane_at:lane_at + 1].astype(I32)
    place = jnp.where(code < group * STRIDE, (code >> 9) * size + (code & (STRIDE - 1)), -1)
    return (place == iota((rows, group * size), 1)).astype(F32).astype(BF16)


def combine_kernel(group, experts, total_tokens, *refs):
    parts, refs = refs[:group], refs[group:]
    info_ref, g_ref, x_ref, frac_ref, y_ref, dl_ref, gr_ref, main_ref, held, sem = refs
    rows, size = g_ref.shape[0], parts[0].shape[0]
    gather_parts(parts, held, sem)
    info = info_ref[...]
    pick = unpick(info, experts + 3, rows, size, group)
    y_tok = jnp.dot(pick, held[...], preferred_element_type=F32)
    prob, lse = info[:, :experts], info[:, experts:experts + 1]
    gate = info[:, experts + 1:experts + 2]
    chosen = (info[:, experts + 2:experts + 3].astype(I32) == iota((rows, experts), 1)).astype(F32)
    grad_out = g_ref[...].astype(F32)
    y_out = (gate * y_tok).astype(BF16)
    y_ref[...] = y_out
    frac = frac_ref[...]
    grad_gate = jnp.sum(grad_out * y_tok, axis=1, keepdims=True)
    mix = jnp.sum(prob * frac, axis=1, keepdims=True)
    dlogits = ((grad_gate * gate) * (chosen - prob)
               + (AUX_WEIGHT * experts / total_tokens) * prob * (frac - mix)
               + (2.0 * Z_WEIGHT / total_tokens) * lse * prob)
    dl = dlogits.astype(BF16)
    dl_ref[...] = dl

    @pl.when(pl.program_id(0) == 0)
    def _():
        gr_ref[...] = jnp.zeros_like(gr_ref)
        main_ref[...] = jnp.zeros_like(main_ref)
    gr_ref[...] += lax.dot_general(dl, x_ref[...], TN, preferred_element_type=F32)
    main_ref[...] += jnp.sum((y_out.astype(F32) * grad_out).reshape(rows // 8, 8, -1), axis=0)


def combine(parts, info, grad_out, x, frac, experts, total_tokens, block=256):
    tokens, dim = x.shape
    group, size = len(parts), parts[0].shape[0]
    return pl.pallas_call(
        functools.partial(combine_kernel, group, experts, total_tokens), grid=(tokens // block,),
        out_shape=(jax.ShapeDtypeStruct((tokens, dim), BF16), jax.ShapeDtypeStruct((tokens, experts), BF16),
                   jax.ShapeDtypeStruct((experts, dim), F32), jax.ShapeDtypeStruct((8, dim), F32)),
        in_specs=[ANY] * group + [pl.BlockSpec((block, 128), lambda i: (i, 0)),
                  pl.BlockSpec((block, dim), lambda i: (i, 0)), pl.BlockSpec((block, dim), lambda i: (i, 0)),
                  pl.BlockSpec((1, experts), lambda i: (0, 0))],
        out_specs=[pl.BlockSpec((block, dim), lambda i: (i, 0)), pl.BlockSpec((block, experts), lambda i: (i, 0)),
                   pl.BlockSpec((experts, dim), lambda i: (0, 0)), pl.BlockSpec((8, dim), lambda i: (0, 0))],
        scratch_shapes=[pltpu.VMEM((group * size, dim), BF16), pltpu.SemaphoreType.DMA((group,))],
        cost_estimate=pl.CostEstimate(flops=2 * group * size * tokens * dim, bytes_accessed=8 * tokens * dim, transcendentals=0),
        name="combine",
    )(*parts, info, grad_out, x, frac)


def finish_kernel(group, experts, *refs):
    parts, (info_ref, dl_ref, w_ref, out_ref, held, sem) = refs[:group], refs[group:]
    rows, size = dl_ref.shape[0], parts[0].shape[0]
    gather_parts(parts, held, sem)
    pick = unpick(info_ref[...], experts + 3, rows, size, group)
    rows_dx = jnp.dot(pick, held[...], preferred_element_type=F32)
    router = lax.dot_general(dl_ref[...], w_ref[...], NT, preferred_element_type=F32)
    out_ref[...] = (rows_dx + router).astype(BF16)


def finish(parts, info, dl, w_router, block=256):
    tokens, experts = dl.shape
    group, (size, dim) = len(parts), parts[0].shape
    return pl.pallas_call(
        functools.partial(finish_kernel, group, experts), grid=(tokens // block,),
        out_shape=jax.ShapeDtypeStruct((tokens, dim), BF16),
        in_specs=[ANY] * group + [pl.BlockSpec((block, 128), lambda i: (i, 0)),
                  pl.BlockSpec((block, experts), lambda i: (i, 0)), pl.BlockSpec((dim, experts), lambda i: (0, 0))],
        out_specs=pl.BlockSpec((block, dim), lambda i: (i, 0)),
        scratch_shapes=[pltpu.VMEM((group * size, dim), BF16), pltpu.SemaphoreType.DMA((group,))],
        cost_estimate=pl.CostEstimate(flops=2 * group * size * tokens * dim, bytes_accessed=4 * tokens * dim, transcendentals=0),
        name="finish",
    )(*parts, info, dl, w_router)


def solution(mesh):
    group = mesh.shape["ep"]

    def swap(parts):
        order = [6, 7, 2, 3, 4, 5, 1]
        got = {0: parts[0]}
        for k in order:
            got[k] = lax.ppermute(parts[k], "ep", [(i, i ^ k) for i in range(group)])
        return [got[k] for k in range(group)]

    def sum_all(part):
        terms = swap([part] * group)
        while len(terms) > 1:
            terms = [a + b for a, b in zip(terms[::2], terms[1::2])]
        return terms[0]

    def device_step(x_tokens, grad_out, w_router, expert_ids, w_in, w_out):
        tokens, dim = x_tokens.shape
        experts = w_router.shape[1]
        own = w_in.shape[0]
        capacity = 5 * tokens // (4 * experts)
        total_tokens = tokens * group
        size = own * capacity

        slot_row, meta = plan(expert_ids.reshape(1, tokens), group, experts, own, capacity)
        table = run_table(meta[0, :group * own], own)
        route_frac = meta[1:2, :experts].astype(F32) / total_tokens

        recv_x = swap(pack(slot_row, x_tokens, group, size))
        grad_y, info, sums = route(x_tokens, grad_out, w_router, expert_ids.reshape(tokens, 1), slot_row.reshape(tokens, 1))
        recv_dy = swap(pack(slot_row, grad_y, group, size))

        held_y, hidden, dense_x = ffn(table, recv_x, None, w_in, w_out, capacity)
        back_y = swap(held_y)
        held_dx, grad_hidden, dense_dy = ffn(table, recv_dy, hidden, w_in, w_out, capacity)
        back_dx = swap(held_dx)
        grad_w_in, grad_w_out = ffn_weights(table, dense_x, dense_dy, hidden, grad_hidden, own, group)

        y_out, dl, router_t, main_rows = combine(back_y, info, grad_out, x_tokens, route_frac, experts, total_tokens)
        everything = sum_all(jnp.concatenate([router_t, jnp.sum(main_rows, axis=0, keepdims=True), sums[:1]], axis=0))
        grad_router = everything[:experts].T
        main_term = jnp.sum(everything[experts])
        aux_loss = experts * jnp.sum(route_frac[0] * everything[experts + 1, :experts]) / total_tokens
        z_loss = everything[experts + 1, experts] / total_tokens
        objective = main_term + AUX_WEIGHT * aux_loss + Z_WEIGHT * z_loss
        grad_x = finish(back_dx, info, dl, w_router)
        return y_out, grad_x, objective, main_term, grad_router, grad_w_in, grad_w_out

    spec_tok = P("ep", None)
    spec_exp = P("ep", None, None)
    return jax.shard_map(device_step, mesh=mesh,
                         in_specs=(spec_tok, spec_tok, P(None, None), P("ep"), spec_exp, spec_exp),
                         out_specs=(spec_tok, spec_tok, P(), P(), P(None, None), spec_exp, spec_exp),
                         check_vma=False)
```

```python
import functools

import jax
import jax.numpy as jnp
from jax import lax
from jax.experimental import pallas as pl
from jax.experimental.pallas import tpu as pltpu
from jax.sharding import PartitionSpec as P

AUX_WEIGHT = 0.01
Z_WEIGHT = 0.001
MESH = pl.DeviceIdType.MESH
GRP = 8
TILE = 256
NOWHERE = 8192.0
F32, BF16, I32 = jnp.float32, jnp.bfloat16, jnp.int32
NT = (((1,), (1,)), ((), ()))
TN = (((0,), (0,)), ((), ()))
ANY = pl.BlockSpec(memory_space=pl.ANY)


def iota(shape, dim):
    return lax.broadcasted_iota(I32, shape, dim)


def plan_kernel(group, experts, own, capacity, ids_ref, tok_ref, meta_ref, sbuf, rbuf, send_sem, recv_sem):
    tokens = ids_ref.shape[1]
    me = lax.axis_index("ep")
    barrier = pltpu.get_barrier_semaphore()
    for k in range(1, group):
        pl.semaphore_signal(barrier, inc=1, device_id=(lax.rem(me + k, group),), device_id_type=MESH)

    onehot = ids_ref[...] == iota((experts, tokens), 0)
    ohb = onehot.astype(F32).astype(BF16)
    counts = lax.dot_general(jnp.ones((8, tokens), BF16), ohb, NT, preferred_element_type=F32)
    sbuf[...] = jnp.zeros_like(sbuf)
    sbuf[:, :experts] = counts
    rbuf[pl.ds(me, 1)] = jnp.zeros((1, 8, 128), F32)
    rbuf[pl.ds(me, 1), :, :experts] = counts[None]

    chunks = tokens // 128
    stacked = jnp.concatenate([ohb[:, c * 128:(c + 1) * 128] for c in range(chunks)], axis=0)
    upper = (iota((128, 128), 0) <= iota((128, 128), 1)).astype(F32).astype(BF16)
    prefix = jnp.dot(stacked, upper, preferred_element_type=F32)

    pl.semaphore_wait(barrier, group - 1)
    copies = []
    for k in range(1, group):
        copy = pltpu.make_async_remote_copy(
            src_ref=sbuf, dst_ref=rbuf.at[me], send_sem=send_sem.at[k - 1], recv_sem=recv_sem.at[k - 1],
            device_id=(lax.rem(me + k, group),), device_id_type=MESH)
        copy.start()
        copies.append(copy)

    carry = jnp.zeros((experts, 1), F32)
    places = []
    for c in range(chunks):
        part = prefix[c * experts:(c + 1) * experts]
        places.append(part + carry)
        carry = carry + part[:, 127:128]
    groups_col = ((jnp.minimum(carry.astype(I32), capacity) + (GRP - 1)) >> 3).astype(F32)
    ahead = iota((experts, experts), 0) > iota((experts, experts), 1)
    base = jnp.dot(ahead.astype(F32).astype(BF16), jnp.broadcast_to(groups_col, (experts, 128)).astype(BF16),
                   preferred_element_type=F32) * GRP
    ids = ids_ref[...].astype(F32)
    for c in range(chunks):
        mask = onehot[:, c * 128:(c + 1) * 128]
        place = jnp.sum(jnp.where(mask, places[c], 0.0), axis=0, keepdims=True) - 1.0
        start = jnp.sum(jnp.where(mask, base, 0.0), axis=0, keepdims=True)
        where = jnp.where(place < capacity, start + place, NOWHERE)
        tok_ref[:, c * 128:(c + 1) * 128] = jnp.concatenate(
            [where, ids[:, c * 128:(c + 1) * 128], jnp.zeros((6, 128), F32)], axis=0)

    for copy in copies:
        copy.wait()

    row, lane = iota((group, 128), 0), iota((group, 128), 1)
    raw = jnp.concatenate([rbuf[s, 0:1, :] for s in range(group)], axis=0).astype(I32)
    groups = (jnp.minimum(raw, capacity) + (GRP - 1)) >> 3
    lane_row = iota((1, 128), 1)
    mine = jnp.sum(jnp.where(row == me, groups, 0), axis=0, keepdims=True)
    zero = jnp.zeros((1, 128), I32)
    held, inside, dense, totals = zero, zero, zero, zero
    sent, sent_at = zero, zero
    columns = [jnp.sum(jnp.where(lane == me * own + l, groups, 0), axis=1, keepdims=True) for l in range(own)]
    starts = [zero[:, :1]] * own
    ahead_col = zero[:, :1]
    for k in range(group):
        other = jnp.bitwise_xor(me, k)
        inner = zero[:, :1]
        for l in range(own):
            size = jnp.sum(jnp.where(row[:, :1] == other, columns[l], 0), axis=0, keepdims=True)
            at = lane_row == k * own + l
            held = jnp.where(at, size, held)
            inside = jnp.where(at, inner, inside)
            dense = jnp.where(at, starts[l], dense)
            inner = inner + size
            starts[l] = starts[l] + size
        to_other = (lane_row >= other * own) & (lane_row < (other + 1) * own)
        sent = jnp.where(lane_row == k, jnp.sum(jnp.where(to_other, mine, 0), axis=1, keepdims=True), sent)
        before = jnp.sum(jnp.where(lane_row < other * own, mine, 0), axis=1, keepdims=True)
        sent_at = jnp.where(lane_row == k, before, sent_at)
    for l in range(own):
        totals = jnp.where(lane_row == l, starts[l], totals)
    sent_all = jnp.broadcast_to(jnp.sum(mine, axis=1, keepdims=True), (1, 128))
    meta_ref[...] = jnp.concatenate([
        held, inside, dense, totals, sent, sent_at, sent_all, jnp.sum(raw, axis=0, keepdims=True)], axis=0)


def plan(ids_row, group, experts, own, capacity):
    tokens = ids_row.shape[1]
    return pl.pallas_call(
        functools.partial(plan_kernel, group, experts, own, capacity),
        out_shape=(jax.ShapeDtypeStruct((8, tokens), F32), jax.ShapeDtypeStruct((8, 128), I32)),
        in_specs=[pl.BlockSpec(memory_space=pltpu.VMEM)],
        out_specs=[pl.BlockSpec(memory_space=pltpu.VMEM)] * 2,
        scratch_shapes=[pltpu.VMEM((8, 128), F32), pltpu.VMEM((group, 8, 128), F32),
                        pltpu.SemaphoreType.DMA((group - 1,)), pltpu.SemaphoreType.DMA((group - 1,))],
        compiler_params=pltpu.CompilerParams(collective_id=0, has_side_effects=True),
        name="plan",
    )(ids_row)


SEND_TILE = 512


def pack_rows(group, meta_ref, tok_ref, rows_ref, outs, dense, sem):
    tokens, dim = rows_ref.shape

    def body(i, _):
        pick = (tok_ref[0:1].astype(I32) - i * SEND_TILE == iota((SEND_TILE, tokens), 0)).astype(F32).astype(BF16)
        rows = jnp.dot(pick, rows_ref[...], preferred_element_type=F32).astype(BF16)
        step = SEND_TILE // GRP
        dense[pl.ds(i * step, step)] = rows.reshape(step, GRP, dim)
        return 0

    lax.fori_loop(0, (meta_ref[6, 0] * GRP + SEND_TILE - 1) // SEND_TILE, body, 0)
    for act in ("start", "wait"):
        for k in range(group):
            size = meta_ref[4, k]

            @pl.when(size > 0)
            def _():
                copy = pltpu.make_async_copy(dense.at[pl.ds(meta_ref[5, k], size)], outs[k].at[pl.ds(0, size)], sem.at[k])
                getattr(copy, act)()


def pack_kernel(group, meta_ref, tok_ref, rows_ref, *refs):
    pack_rows(group, meta_ref, tok_ref, rows_ref, refs[:group], *refs[group:])


def send_tiles(tokens, experts):
    return -(-(tokens + experts * (GRP - 1)) // SEND_TILE) * (SEND_TILE // GRP)


def pack(meta, tok, rows, group, size, experts):
    tokens, dim = rows.shape
    return pl.pallas_call(
        functools.partial(pack_kernel, group),
        out_shape=[jax.ShapeDtypeStruct((size // GRP, GRP, dim), BF16)] * group,
        in_specs=[pl.BlockSpec(memory_space=pltpu.SMEM)] + [pl.BlockSpec(memory_space=pltpu.VMEM)] * 2,
        out_specs=[ANY] * group,
        scratch_shapes=[pltpu.VMEM((send_tiles(tokens, experts), GRP, dim), BF16), pltpu.SemaphoreType.DMA((group,))],
        cost_estimate=pl.CostEstimate(flops=2 * tokens * tokens * dim, bytes_accessed=4 * tokens * dim, transcendentals=0),
        name="pack",
    )(meta, tok, rows)


def route_kernel(group, experts, block, meta_ref, tok_ref, x_ref, g_ref, w_ref, after_ref, *refs):
    outs, (info_ref, sums_ref, dy, dense, sem) = refs[:group], refs[group:]
    del after_ref
    sums_ref[...] = jnp.zeros_like(sums_ref)
    tokens = x_ref.shape[0]
    for i in range(tokens // block):
        at = pl.ds(i * block, block)
        logits = lax.dot_general(x_ref[at], w_ref[...], NT, preferred_element_type=F32)
        top = jnp.max(logits, axis=1, keepdims=True)
        lse = top + jnp.log(jnp.sum(jnp.exp(logits - top), axis=1, keepdims=True))
        prob = jnp.exp(logits - lse)
        columns = tok_ref[:, i * block:(i + 1) * block].T
        chosen = columns[:, 1:2].astype(I32) == iota((block, experts), 1)
        gate = jnp.sum(jnp.where(chosen, prob, 0.0), axis=1, keepdims=True)
        dy[at] = (gate * g_ref[at].astype(F32)).astype(BF16)
        info_ref[at, :experts] = prob
        info_ref[at, experts:experts + 1] = lse
        info_ref[at, experts + 1:experts + 2] = gate
        info_ref[at, experts + 2:experts + 3] = columns[:, 1:2]
        info_ref[at, experts + 3:experts + 4] = columns[:, 0:1]
        sums_ref[0:1, :experts] += jnp.sum(prob, axis=0, keepdims=True)
        sums_ref[0:1, experts:experts + 1] += jnp.sum(lse * lse, axis=0, keepdims=True)
    pack_rows(group, meta_ref, tok_ref, dy, outs, dense, sem)


def route(meta, tok, x, grad_out, router_t, after, group, size, block=512):
    tokens, dim = x.shape
    experts = router_t.shape[0]
    vmem = pl.BlockSpec(memory_space=pltpu.VMEM)
    result = pl.pallas_call(
        functools.partial(route_kernel, group, experts, block),
        out_shape=[jax.ShapeDtypeStruct((size // GRP, GRP, dim), BF16)] * group + [
            jax.ShapeDtypeStruct((tokens, 128), F32), jax.ShapeDtypeStruct((8, dim), F32)],
        in_specs=[pl.BlockSpec(memory_space=pltpu.SMEM)] + [vmem] * 4 + [ANY],
        out_specs=[ANY] * group + [vmem] * 2,
        scratch_shapes=[pltpu.VMEM((tokens, dim), BF16), pltpu.VMEM((send_tiles(tokens, experts), GRP, dim), BF16),
                        pltpu.SemaphoreType.DMA((group,))],
        cost_estimate=pl.CostEstimate(flops=3 * tokens * tokens * dim, bytes_accessed=6 * tokens * dim, transcendentals=0),
        name="route",
    )(meta, tok, x, grad_out, router_t, after)
    return result[:group], result[group], result[group + 1]


class Runs:
    def __init__(self, ref, group, own):
        self.ref, self.group, self.own = ref, group, own

    def get(self, kind, k, e):
        return self.ref[kind, k * self.own + e]

    def size(self, k, e):
        return self.get(0, k, e)

    def inside(self, k, e):
        return self.get(1, k, e)

    def dense(self, k, e):
        return self.get(2, k, e)

    def rows(self, e):
        return self.ref[3, e] * GRP

    def tiles(self, e):
        return (self.rows(e) + (TILE - 1)) // TILE


def each_run(runs, e, act, make):
    for k in range(runs.group):
        size = runs.size(k, e)

        @pl.when(size > 0)
        def _():
            getattr(make(k, size), act)()


def fill(runs, e, parts, dense, sem, act):
    def make(k, size):
        return pltpu.make_async_copy(parts[k].at[pl.ds(runs.inside(k, e), size)],
                                     dense.at[e, pl.ds(runs.dense(k, e), size)], sem.at[e, k])
    each_run(runs, e, act, make)


def drain(runs, e, dense, parts, sem, act):
    def make(k, size):
        return pltpu.make_async_copy(dense.at[e, pl.ds(runs.dense(k, e), size)],
                                     parts[k].at[pl.ds(runs.inside(k, e), size)], sem.at[e, k])
    each_run(runs, e, act, make)


def ffn_frame(runs, ins, outs, dense_in, dense_out, in_sem, out_sem):
    e, step = pl.program_id(0), pl.program_id(1)
    last = pl.num_programs(1) - 1

    @pl.when((e == 0) & (step == 0))
    def _():
        for i in range(runs.own):
            fill(runs, i, ins, dense_in, in_sem, "start")

    for i in range(runs.own):
        @pl.when((e == i) & (step == 0))
        def _():
            fill(runs, i, ins, dense_in, in_sem, "wait")

    def after():
        for i in range(runs.own):
            @pl.when((e == i) & (step == last))
            def _():
                drain(runs, i, dense_out, outs, out_sem, "start")

        @pl.when((e == runs.own - 1) & (step == last))
        def _():
            for i in range(runs.own):
                drain(runs, i, dense_out, outs, out_sem, "wait")
    return after


def each_tile(tiles, work):
    lax.fori_loop(0, tiles // 2, lambda i, _: (work(i * 2, 2 * TILE), 0)[1], 0)

    @pl.when(tiles % 2 == 1)
    def _():
        work(tiles - 1, TILE)


def accumulate(step, last, acc, at, part, store):
    @pl.when(step == 0)
    def _():
        acc[at] = part

    @pl.when((step > 0) & (step < last))
    def _():
        acc[at] += part

    @pl.when(step == last)
    def _():
        store((acc[at] + part).astype(BF16))


def ffn_kernel(group, backward, table_ref, *refs):
    ins, refs = refs[:group], refs[group:]
    if backward:
        h_ref, refs = refs[0], refs[1:]
    win_ref, wout_ref = refs[:2]
    outs, refs = refs[2:2 + group], refs[2 + group:]
    mid_ref, clean_ref, acc, dense_in, dense_out, in_sem, out_sem = refs
    own = dense_in.shape[0]
    runs = Runs(table_ref, group, own)
    e, step, last = pl.program_id(0), pl.program_id(1), pl.num_programs(1) - 1
    dim = win_ref.shape[1]
    after = ffn_frame(runs, ins, outs, dense_in, dense_out, in_sem, out_sem)
    rows = runs.rows(e)

    def work(tile, size):
        at = pl.ds(pl.multiple_of(tile * TILE, TILE), size)
        of = pl.ds(tile * (TILE // GRP), size // GRP)

        @pl.when(step == 0)
        def _():
            fresh = dense_in[e, of].reshape(size, dim)
            clean_ref[at] = jnp.where(tile * TILE + iota((size, dim), 0) < rows, fresh, jnp.zeros_like(fresh))

        if backward:
            full = lax.dot_general(clean_ref[at], wout_ref[0], NT, preferred_element_type=F32)
            mid = jnp.where(h_ref[at].astype(F32) > 0.0, full, 0.0).astype(BF16)
            part = lax.dot_general(mid, win_ref[0], NT, preferred_element_type=F32)
        else:
            mid = jnp.maximum(jnp.dot(clean_ref[at], win_ref[0], preferred_element_type=F32), 0.0).astype(BF16)
            part = jnp.dot(mid, wout_ref[0], preferred_element_type=F32)
        mid_ref[at] = mid

        def store(value):
            dense_out[e, of] = value.reshape(size // GRP, GRP, dim)
        accumulate(step, last, acc, at, part, store)

    each_tile(runs.tiles(e), work)
    after()


def ffn(table, parts, hidden, w_in, w_out, capacity, block=1024):
    group = len(parts)
    own, dim, ff = w_in.shape
    held = group * capacity
    size = parts[0].shape[0]
    extra = [] if hidden is None else [hidden]
    result = pl.pallas_call(
        functools.partial(ffn_kernel, group, hidden is not None),
        out_shape=[jax.ShapeDtypeStruct((size, GRP, dim), BF16)] * group + [
            jax.ShapeDtypeStruct((own * held, ff), BF16), jax.ShapeDtypeStruct((own * held, dim), BF16)],
        grid_spec=pltpu.PrefetchScalarGridSpec(
            num_scalar_prefetch=1, grid=(own, ff // block),
            in_specs=[ANY] * group + [pl.BlockSpec((held, block), lambda e, f, t: (e, f))] * len(extra) + [
                pl.BlockSpec((1, dim, block), lambda e, f, t: (e, 0, f)),
                pl.BlockSpec((1, block, dim), lambda e, f, t: (e, f, 0))],
            out_specs=[ANY] * group + [pl.BlockSpec((held, block), lambda e, f, t: (e, f)),
                                       pl.BlockSpec((held, dim), lambda e, f, t: (e, 0))],
            scratch_shapes=[pltpu.VMEM((held, dim), F32),
                            pltpu.VMEM((own, held // GRP, GRP, dim), BF16), pltpu.VMEM((own, held // GRP, GRP, dim), BF16),
                            pltpu.SemaphoreType.DMA((own, group)), pltpu.SemaphoreType.DMA((own, group))]),
        cost_estimate=pl.CostEstimate(flops=3 * own * held * dim * ff, bytes_accessed=40 << 20, transcendentals=0),
        name="ffn_forward" if hidden is None else "ffn_backward",
    )(table, *parts, *extra, w_in, w_out)
    return result[:group], result[group], result[group + 1]


def ffn_weights(table, x, dy, hidden, grad_hidden, own, group, block=1024):
    dim, ff = x.shape[1], hidden.shape[1]
    rows = x.shape[0] // own

    def kernel(table_ref, *refs):
        r = Runs(table_ref, group, own)
        return weights_body(r, *refs)

    return pl.pallas_call(
        kernel,
        out_shape=(jax.ShapeDtypeStruct((own, dim, ff), F32), jax.ShapeDtypeStruct((own, ff, dim), F32)),
        grid_spec=pltpu.PrefetchScalarGridSpec(
            num_scalar_prefetch=1, grid=(own, ff // block),
            in_specs=[pl.BlockSpec((rows, dim), lambda e, f, t: (e, 0)),
                      pl.BlockSpec((rows, dim), lambda e, f, t: (e, 0)),
                      pl.BlockSpec((rows, block), lambda e, f, t: (e, f)),
                      pl.BlockSpec((rows, block), lambda e, f, t: (e, f))],
            out_specs=[pl.BlockSpec((1, dim, block), lambda e, f, t: (e, 0, f)),
                       pl.BlockSpec((1, block, dim), lambda e, f, t: (e, f, 0))]),
        cost_estimate=pl.CostEstimate(flops=3 * own * rows * dim * ff, bytes_accessed=60 << 20, transcendentals=0),
        name="ffn_weights",
    )(table, x, dy, hidden, grad_hidden)


def weights_body(runs, x_ref, dy_ref, h_ref, dh_ref, gin_ref, gout_ref):
    tiles = runs.tiles(pl.program_id(0))

    @pl.when(tiles == 0)
    def _():
        gin_ref[...] = jnp.zeros_like(gin_ref)
        gout_ref[...] = jnp.zeros_like(gout_ref)

    def work(tile, size):
        at = pl.ds(pl.multiple_of(tile * TILE, TILE), size)
        gin = lax.dot_general(x_ref[at], dh_ref[at], TN, preferred_element_type=F32)
        gout = lax.dot_general(h_ref[at], dy_ref[at], TN, preferred_element_type=F32)

        @pl.when(tile == 0)
        def _():
            gin_ref[0] = gin
            gout_ref[0] = gout

        @pl.when(tile > 0)
        def _():
            gin_ref[0] += gin
            gout_ref[0] += gout

    each_tile(tiles, work)


def gather_parts(group, meta_ref, parts, held, sem):
    @pl.when(pl.program_id(0) == 0)
    def _():
        for act in ("start", "wait"):
            for k in range(group):
                size = meta_ref[4, k]

                @pl.when(size > 0)
                def _():
                    copy = pltpu.make_async_copy(parts[k].at[pl.ds(0, size)], held.at[pl.ds(meta_ref[5, k], size)], sem.at[k])
                    getattr(copy, act)()

        def blank(i, _):
            held[i] = jnp.zeros(held.shape[1:], held.dtype)
            return 0
        lax.fori_loop(meta_ref[6, 0], held.shape[0], blank, 0)


def unpick(meta_ref, info_ref, lane_at, held, out):
    rows, (groups, _, dim) = info_ref.shape[0], held.shape
    place = info_ref[:, lane_at:lane_at + 1].astype(I32)
    few = groups * 3 // 5 // 32 * 32

    def pick(count):
        size = count * GRP
        onehot = (place == iota((rows, size), 1)).astype(F32).astype(BF16)
        out[...] = jnp.dot(onehot, held[pl.ds(0, count)].reshape(size, dim), preferred_element_type=F32)

    @pl.when(meta_ref[6, 0] <= few)
    def _():
        pick(few)

    @pl.when(meta_ref[6, 0] > few)
    def _():
        pick(groups)


def combine_kernel(group, experts, total_tokens, *refs):
    meta_ref, parts, refs = refs[0], refs[1:1 + group], refs[1 + group:]
    info_ref, g_ref, x_ref, count_ref, y_ref, dl_ref, gr_ref, main_ref, held, got, sem = refs
    rows = g_ref.shape[0]
    gather_parts(group, meta_ref, parts, held, sem)
    info = info_ref[...]
    unpick(meta_ref, info_ref, experts + 3, held, got)
    y_tok = got[...]
    prob, lse = info[:, :experts], info[:, experts:experts + 1]
    gate = info[:, experts + 1:experts + 2]
    chosen = (info[:, experts + 2:experts + 3].astype(I32) == iota((rows, experts), 1)).astype(F32)
    grad_out = g_ref[...].astype(F32)
    y_out = (gate * y_tok).astype(BF16)
    y_ref[...] = y_out
    frac = count_ref[7:8, :experts].astype(F32) / total_tokens
    grad_gate = jnp.sum(grad_out * y_tok, axis=1, keepdims=True)
    mix = jnp.sum(prob * frac, axis=1, keepdims=True)
    dlogits = ((grad_gate * gate) * (chosen - prob)
               + (AUX_WEIGHT * experts / total_tokens) * prob * (frac - mix)
               + (2.0 * Z_WEIGHT / total_tokens) * lse * prob)
    dl = dlogits.astype(BF16)
    dl_ref[...] = dl

    @pl.when(pl.program_id(0) == 0)
    def _():
        gr_ref[...] = jnp.zeros_like(gr_ref)
        main_ref[...] = jnp.zeros_like(main_ref)
    gr_ref[...] += lax.dot_general(dl, x_ref[...], TN, preferred_element_type=F32)
    main_ref[...] += jnp.sum((y_out.astype(F32) * grad_out).reshape(rows // 8, 8, -1), axis=0)


def combine(meta, parts, info, grad_out, x, experts, total_tokens, block=512):
    tokens, dim = x.shape
    group = len(parts)
    return pl.pallas_call(
        functools.partial(combine_kernel, group, experts, total_tokens), grid=(tokens // block,),
        out_shape=(jax.ShapeDtypeStruct((tokens, dim), BF16), jax.ShapeDtypeStruct((tokens, experts), BF16),
                   jax.ShapeDtypeStruct((experts, dim), F32), jax.ShapeDtypeStruct((8, dim), F32)),
        in_specs=[pl.BlockSpec(memory_space=pltpu.SMEM)] + [ANY] * group + [pl.BlockSpec((block, 128), lambda i: (i, 0)),
                  pl.BlockSpec((block, dim), lambda i: (i, 0)), pl.BlockSpec((block, dim), lambda i: (i, 0)),
                  pl.BlockSpec((8, 128), lambda i: (0, 0))],
        out_specs=[pl.BlockSpec((block, dim), lambda i: (i, 0)), pl.BlockSpec((block, experts), lambda i: (i, 0)),
                   pl.BlockSpec((experts, dim), lambda i: (0, 0)), pl.BlockSpec((8, dim), lambda i: (0, 0))],
        scratch_shapes=[pltpu.VMEM((send_tiles(tokens, experts), GRP, dim), BF16), pltpu.VMEM((block, dim), F32),
                        pltpu.SemaphoreType.DMA((group,))],
        cost_estimate=pl.CostEstimate(flops=2 * tokens * tokens * dim, bytes_accessed=8 * tokens * dim, transcendentals=0),
        name="combine",
    )(meta, *parts, info, grad_out, x, meta)


def finish_kernel(group, experts, *refs):
    meta_ref, parts, (info_ref, dl_ref, w_ref, out_ref, held, got, sem) = refs[0], refs[1:1 + group], refs[1 + group:]
    gather_parts(group, meta_ref, parts, held, sem)
    unpick(meta_ref, info_ref, experts + 3, held, got)
    router = jnp.dot(dl_ref[...], w_ref[...], preferred_element_type=F32)
    out_ref[...] = (got[...] + router).astype(BF16)


def finish(meta, parts, info, dl, router_t, block=512):
    tokens, experts = dl.shape
    group, dim = len(parts), router_t.shape[1]
    return pl.pallas_call(
        functools.partial(finish_kernel, group, experts), grid=(tokens // block,),
        out_shape=jax.ShapeDtypeStruct((tokens, dim), BF16),
        in_specs=[pl.BlockSpec(memory_space=pltpu.SMEM)] + [ANY] * group + [pl.BlockSpec((block, 128), lambda i: (i, 0)),
                  pl.BlockSpec((block, experts), lambda i: (i, 0)), pl.BlockSpec((experts, dim), lambda i: (0, 0))],
        out_specs=pl.BlockSpec((block, dim), lambda i: (i, 0)),
        scratch_shapes=[pltpu.VMEM((send_tiles(tokens, experts), GRP, dim), BF16), pltpu.VMEM((block, dim), F32),
                        pltpu.SemaphoreType.DMA((group,))],
        cost_estimate=pl.CostEstimate(flops=2 * tokens * tokens * dim, bytes_accessed=4 * tokens * dim, transcendentals=0),
        name="finish",
    )(meta, *parts, info, dl, router_t)


def solution(mesh):
    group = mesh.shape["ep"]

    def swap(parts):
        order = [6, 7, 2, 3, 4, 5, 1]
        got = {0: parts[0]}
        for k in order:
            got[k] = lax.ppermute(parts[k], "ep", [(i, i ^ k) for i in range(group)])
        return [got[k] for k in range(group)]

    def sum_all(part):
        terms = swap([part] * group)
        while len(terms) > 1:
            terms = [a + b for a, b in zip(terms[::2], terms[1::2])]
        return terms[0]

    def device_step(x_tokens, grad_out, w_router, expert_ids, w_in, w_out):
        tokens, dim = x_tokens.shape
        experts = w_router.shape[1]
        own = w_in.shape[0]
        capacity = 5 * tokens // (4 * experts)
        total_tokens = tokens * group
        size = own * capacity

        router_t = w_router.T
        tok, meta = plan(expert_ids.reshape(1, tokens), group, experts, own, capacity)
        send_x = pack(meta, tok, x_tokens, group, size, experts)
        recv_x = swap(send_x)
        send_dy, info, sums = route(meta, tok, x_tokens, grad_out, router_t, send_x[0], group, size)
        recv_dy = swap(send_dy)

        held_y, hidden, dense_x = ffn(meta, recv_x, None, w_in, w_out, capacity)
        back_y = swap(held_y)
        held_dx, grad_hidden, dense_dy = ffn(meta, recv_dy, hidden, w_in, w_out, capacity)
        back_dx = swap(held_dx)
        grad_w_in, grad_w_out = ffn_weights(meta, dense_x, dense_dy, hidden, grad_hidden, own, group)

        y_out, dl, grad_router_t, main_rows = combine(meta, back_y, info, grad_out, x_tokens, experts, total_tokens)
        everything = sum_all(jnp.concatenate([grad_router_t, jnp.sum(main_rows, axis=0, keepdims=True), sums[:1]], axis=0))
        route_frac = meta[7:8, :experts].astype(F32) / total_tokens
        grad_router = everything[:experts].T
        main_term = jnp.sum(everything[experts])
        aux_loss = experts * jnp.sum(route_frac[0] * everything[experts + 1, :experts]) / total_tokens
        z_loss = everything[experts + 1, experts] / total_tokens
        objective = main_term + AUX_WEIGHT * aux_loss + Z_WEIGHT * z_loss
        grad_x = finish(meta, back_dx, info, dl, router_t)
        return y_out, grad_x, objective, main_term, grad_router, grad_w_in, grad_w_out

    spec_tok = P("ep", None)
    spec_exp = P("ep", None, None)
    return jax.shard_map(device_step, mesh=mesh,
                         in_specs=(spec_tok, spec_tok, P(None, None), P("ep"), spec_exp, spec_exp),
                         out_specs=(spec_tok, spec_tok, P(), P(), P(None, None), spec_exp, spec_exp),
                         check_vma=False)
```

```python
import functools

import jax
import jax.numpy as jnp
from jax import lax
from jax.experimental import pallas as pl
from jax.experimental.pallas import tpu as pltpu
from jax.sharding import PartitionSpec as P

AUX_WEIGHT = 0.01
Z_WEIGHT = 0.001
MESH = pl.DeviceIdType.MESH
GRP = 8
TILE = 256
NOWHERE = 8192.0
F32, BF16, I32 = jnp.float32, jnp.bfloat16, jnp.int32
NT = (((1,), (1,)), ((), ()))
TN = (((0,), (0,)), ((), ()))
ANY = pl.BlockSpec(memory_space=pl.ANY)


def iota(shape, dim):
    return lax.broadcasted_iota(I32, shape, dim)


def places(experts, own, capacity, ids, tok_ref, mine_ref, count_ref):
    tokens = ids.shape[1]
    me = lax.axis_index("ep")
    onehot = ids == iota((experts, tokens), 0)
    ohb = onehot.astype(F32).astype(BF16)
    counts = lax.dot_general(jnp.ones((8, tokens), BF16), ohb, NT, preferred_element_type=F32)
    count_ref[...] = jnp.zeros_like(count_ref)
    count_ref[:, :experts] = counts
    lane = iota((8, experts), 1)
    groups = (jnp.minimum(counts.astype(I32), capacity) + (GRP - 1)) >> 3
    sent_all = jnp.sum(groups, axis=1, keepdims=True)
    lane_row, row = iota((8, 128), 1), iota((8, 128), 0)
    sent, start = jnp.zeros((8, 128), I32), jnp.zeros((8, 128), I32)
    for k in range(experts // own):
        other = jnp.bitwise_xor(me, k)
        to_other = jnp.sum(jnp.where((lane >= other * own) & (lane < (other + 1) * own), groups, 0), axis=1, keepdims=True)
        before = jnp.sum(jnp.where(lane < other * own, groups, 0), axis=1, keepdims=True)
        sent = jnp.where(lane_row == k, to_other, sent)
        start = jnp.where(lane_row == k, before, start)
    mine_ref[...] = jnp.where(row == 0, sent, jnp.where(row == 1, start, jnp.where(row == 2, sent_all, me)))

    chunks = tokens // 128
    stacked = jnp.concatenate([ohb[:, c * 128:(c + 1) * 128] for c in range(chunks)], axis=0)
    upper = (iota((128, 128), 0) <= iota((128, 128), 1)).astype(F32).astype(BF16)
    prefix = jnp.dot(stacked, upper, preferred_element_type=F32)
    carry = jnp.zeros((experts, 1), F32)
    ranks = []
    for c in range(chunks):
        part = prefix[c * experts:(c + 1) * experts]
        ranks.append(part + carry)
        carry = carry + part[:, 127:128]
    groups_col = ((jnp.minimum(carry.astype(I32), capacity) + (GRP - 1)) >> 3).astype(F32)
    ahead = iota((experts, experts), 0) > iota((experts, experts), 1)
    base = jnp.dot(ahead.astype(F32).astype(BF16), jnp.broadcast_to(groups_col, (experts, 128)).astype(BF16),
                   preferred_element_type=F32) * GRP
    idf = ids.astype(F32)
    for c in range(chunks):
        mask = onehot[:, c * 128:(c + 1) * 128]
        place = jnp.sum(jnp.where(mask, ranks[c], 0.0), axis=0, keepdims=True) - 1.0
        first = jnp.sum(jnp.where(mask, base, 0.0), axis=0, keepdims=True)
        where = jnp.where(place < capacity, first + place, NOWHERE)
        tok_ref[:, c * 128:(c + 1) * 128] = jnp.concatenate(
            [where, idf[:, c * 128:(c + 1) * 128], jnp.zeros((6, 128), F32)], axis=0)


def tally_kernel(group, own, capacity, count_ref, after_ref, meta_ref, rbuf, send_sem, recv_sem):
    del after_ref
    me = lax.axis_index("ep")
    barrier = pltpu.get_barrier_semaphore()
    for k in range(1, group):
        pl.semaphore_signal(barrier, inc=1, device_id=(lax.rem(me + k, group),), device_id_type=MESH)
    pl.semaphore_wait(barrier, group - 1)
    copies = []
    for k in range(1, group):
        copy = pltpu.make_async_remote_copy(
            src_ref=count_ref, dst_ref=rbuf.at[me], send_sem=send_sem.at[k - 1], recv_sem=recv_sem.at[k - 1],
            device_id=(lax.rem(me + k, group),), device_id_type=MESH)
        copy.start()
        copies.append(copy)
    rbuf[pl.ds(me, 1)] = count_ref[...][None]
    for copy in copies:
        copy.wait()

    row, lane = iota((group, 128), 0), iota((group, 128), 1)
    raw = jnp.concatenate([rbuf[s, 0:1, :] for s in range(group)], axis=0).astype(I32)
    groups = (jnp.minimum(raw, capacity) + (GRP - 1)) >> 3
    lane_row = iota((1, 128), 1)
    zero = jnp.zeros((1, 128), I32)
    held, inside, dense, totals = zero, zero, zero, zero
    columns = [jnp.sum(jnp.where(lane == me * own + l, groups, 0), axis=1, keepdims=True) for l in range(own)]
    starts = [zero[:, :1]] * own
    for k in range(group):
        other = jnp.bitwise_xor(me, k)
        inner = zero[:, :1]
        for l in range(own):
            size = jnp.sum(jnp.where(row[:, :1] == other, columns[l], 0), axis=0, keepdims=True)
            at = lane_row == k * own + l
            held = jnp.where(at, size, held)
            inside = jnp.where(at, inner, inside)
            dense = jnp.where(at, starts[l], dense)
            inner = inner + size
            starts[l] = starts[l] + size
    worst = zero[:, :1]
    for d in range(group):
        part = jnp.sum(jnp.where((lane >= d * own) & (lane < (d + 1) * own), groups, 0), axis=1, keepdims=True)
        worst = jnp.maximum(worst, jnp.max(part, axis=0, keepdims=True))
    for l in range(own):
        totals = jnp.where(lane_row == l, starts[l], totals)
    meta_ref[...] = jnp.concatenate([
        held, inside, dense, totals, jnp.broadcast_to(worst, (1, 128)), jnp.sum(raw, axis=0, keepdims=True),
        jnp.full((1, 128), me, I32), zero], axis=0)


def tally(counts, after, group, own, capacity):
    return pl.pallas_call(
        functools.partial(tally_kernel, group, own, capacity),
        out_shape=jax.ShapeDtypeStruct((8, 128), I32),
        in_specs=[pl.BlockSpec(memory_space=pltpu.VMEM), ANY],
        out_specs=pl.BlockSpec(memory_space=pltpu.VMEM),
        scratch_shapes=[pltpu.VMEM((group, 8, 128), F32),
                        pltpu.SemaphoreType.DMA((group - 1,)), pltpu.SemaphoreType.DMA((group - 1,))],
        compiler_params=pltpu.CompilerParams(collective_id=0, has_side_effects=True),
        cost_estimate=pl.CostEstimate(flops=1000000000, bytes_accessed=65536, transcendentals=0),
        name="tally",
    )(counts, after)


class Parts:
    def __init__(self, mains, over, me):
        self.mains, self.over, self.me, self.fit = mains, over, me, mains[0].shape[0]

    def spans(self, k, start, size):
        first = jnp.clip(self.fit - start, 0, size)
        rest = size - first
        yield self.mains[k].at[pl.ds(start, first)], 0, first
        yield self.over.at[jnp.bitwise_xor(self.me, k), pl.ds(jnp.maximum(start - self.fit, 0), rest)], first, rest


def move(parts, k, start, size, rows_at, sem, act, inward):
    for i, (ref, before, count) in enumerate(parts.spans(k, start, size)):
        @pl.when(count > 0)
        def _():
            other = rows_at(before, count)
            pair = (ref, other) if inward else (other, ref)
            getattr(pltpu.make_async_copy(*pair, sem.at[i]), act)()


SEND_TILE = 512


def pack_rows(group, mine_ref, tok_ref, rows_ref, parts, dense, sem):
    tokens, dim = rows_ref.shape

    def body(i, _):
        pick = (tok_ref[0:1].astype(I32) - i * SEND_TILE == iota((SEND_TILE, tokens), 0)).astype(F32).astype(BF16)
        rows = jnp.dot(pick, rows_ref[...], preferred_element_type=F32).astype(BF16)
        step = SEND_TILE // GRP
        dense[pl.ds(i * step, step)] = rows.reshape(step, GRP, dim)
        return 0

    lax.fori_loop(0, (mine_ref[2, 0] * GRP + SEND_TILE - 1) // SEND_TILE, body, 0)
    for act in ("start", "wait"):
        for k in range(group):
            move(parts, k, 0, mine_ref[0, k],
                 lambda before, count, k=k: dense.at[pl.ds(mine_ref[1, k] + before, count)], sem.at[k], act, False)


def pack_kernel(group, experts, own, capacity, ids_ref, rows_ref, *refs):
    mains, over, (tok_ref, mine_ref, count_ref, mine, dense, sem, mine_sem) = refs[:group], refs[group], refs[group + 1:]
    places(experts, own, capacity, ids_ref[...], tok_ref, mine_ref, count_ref)
    copy = pltpu.make_async_copy(mine_ref, mine, mine_sem)
    copy.start()
    copy.wait()
    pack_rows(group, mine, tok_ref, rows_ref, Parts(mains, over, mine[3, 0]), dense, sem)


def part_shapes(group, fit, spill, dim):
    return [jax.ShapeDtypeStruct((fit, GRP, dim), BF16)] * group + [jax.ShapeDtypeStruct((group, spill, GRP, dim), BF16)]


def send_tiles(tokens, experts):
    return -(-(tokens + experts * (GRP - 1)) // SEND_TILE) * (SEND_TILE // GRP)


def pack(ids_row, rows, group, experts, capacity, fit, spill):
    tokens, dim = rows.shape
    vmem = pl.BlockSpec(memory_space=pltpu.VMEM)
    result = pl.pallas_call(
        functools.partial(pack_kernel, group, experts, experts // group, capacity),
        out_shape=part_shapes(group, fit, spill, dim) + [
            jax.ShapeDtypeStruct((8, tokens), F32), jax.ShapeDtypeStruct((8, 128), I32), jax.ShapeDtypeStruct((8, 128), F32)],
        in_specs=[vmem] * 2,
        out_specs=[ANY] * (group + 1) + [vmem] * 3,
        scratch_shapes=[pltpu.SMEM((8, 128), I32), pltpu.VMEM((send_tiles(tokens, experts), GRP, dim), BF16),
                        pltpu.SemaphoreType.DMA((group, 2)), pltpu.SemaphoreType.DMA],
        cost_estimate=pl.CostEstimate(flops=2 * tokens * tokens * dim, bytes_accessed=4 * tokens * dim, transcendentals=0),
        name="pack",
    )(ids_row, rows)
    return result[:group + 1], *result[group + 1:]


def route_kernel(group, experts, block, mine_ref, tok_ref, x_ref, g_ref, w_ref, after_ref, *refs):
    mains, over, (info_ref, sums_ref, dy, dense, sem) = refs[:group], refs[group], refs[group + 1:]
    del after_ref
    sums_ref[...] = jnp.zeros_like(sums_ref)
    tokens = x_ref.shape[0]
    for i in range(tokens // block):
        at = pl.ds(i * block, block)
        logits = lax.dot_general(x_ref[at], w_ref[...], NT, preferred_element_type=F32)
        top = jnp.max(logits, axis=1, keepdims=True)
        lse = top + jnp.log(jnp.sum(jnp.exp(logits - top), axis=1, keepdims=True))
        prob = jnp.exp(logits - lse)
        columns = tok_ref[:, i * block:(i + 1) * block].T
        chosen = columns[:, 1:2].astype(I32) == iota((block, experts), 1)
        gate = jnp.sum(jnp.where(chosen, prob, 0.0), axis=1, keepdims=True)
        dy[at] = (gate * g_ref[at].astype(F32)).astype(BF16)
        info_ref[at, :experts] = prob
        info_ref[at, experts:experts + 1] = lse
        info_ref[at, experts + 1:experts + 2] = gate
        info_ref[at, experts + 2:experts + 3] = columns[:, 1:2]
        info_ref[at, experts + 3:experts + 4] = columns[:, 0:1]
        sums_ref[0:1, :experts] += jnp.sum(prob, axis=0, keepdims=True)
        sums_ref[0:1, experts:experts + 1] += jnp.sum(lse * lse, axis=0, keepdims=True)
    pack_rows(group, mine_ref, tok_ref, dy, Parts(mains, over, mine_ref[3, 0]), dense, sem)


def route(mine, tok, x, grad_out, router_t, after, group, fit, spill, block=512):
    tokens, dim = x.shape
    experts = router_t.shape[0]
    vmem = pl.BlockSpec(memory_space=pltpu.VMEM)
    result = pl.pallas_call(
        functools.partial(route_kernel, group, experts, block),
        out_shape=part_shapes(group, fit, spill, dim) + [
            jax.ShapeDtypeStruct((tokens, 128), F32), jax.ShapeDtypeStruct((8, dim), F32)],
        in_specs=[pl.BlockSpec(memory_space=pltpu.SMEM)] + [vmem] * 4 + [ANY],
        out_specs=[ANY] * (group + 1) + [vmem] * 2,
        scratch_shapes=[pltpu.VMEM((tokens, dim), BF16), pltpu.VMEM((send_tiles(tokens, experts), GRP, dim), BF16),
                        pltpu.SemaphoreType.DMA((group, 2))],
        cost_estimate=pl.CostEstimate(flops=3 * tokens * tokens * dim, bytes_accessed=6 * tokens * dim, transcendentals=0),
        name="route",
    )(mine, tok, x, grad_out, router_t, after)
    return result[:group + 1], result[group + 1], result[group + 2]


class Runs:
    def __init__(self, ref, group, own):
        self.ref, self.group, self.own = ref, group, own

    def get(self, kind, k, e):
        return self.ref[kind, k * self.own + e]

    def size(self, k, e):
        return self.get(0, k, e)

    def inside(self, k, e):
        return self.get(1, k, e)

    def dense(self, k, e):
        return self.get(2, k, e)

    def rows(self, e):
        return self.ref[3, e] * GRP

    def tiles(self, e):
        return (self.rows(e) + (TILE - 1)) // TILE


def fill(runs, e, parts, dense, sem, act):
    for k in range(runs.group):
        move(parts, k, runs.inside(k, e), runs.size(k, e),
             lambda before, count, k=k: dense.at[e, pl.ds(runs.dense(k, e) + before, count)], sem.at[e, k], act, True)


def drain(runs, e, dense, parts, sem, act):
    for k in range(runs.group):
        move(parts, k, runs.inside(k, e), runs.size(k, e),
             lambda before, count, k=k: dense.at[e, pl.ds(runs.dense(k, e) + before, count)], sem.at[e, k], act, False)


def ffn_frame(runs, ins, outs, dense_in, dense_out, in_sem, out_sem):
    e, step = pl.program_id(0), pl.program_id(1)
    last = pl.num_programs(1) - 1

    @pl.when((e == 0) & (step == 0))
    def _():
        for i in range(runs.own):
            fill(runs, i, ins, dense_in, in_sem, "start")

    for i in range(runs.own):
        @pl.when((e == i) & (step == 0))
        def _():
            fill(runs, i, ins, dense_in, in_sem, "wait")

    def after():
        for i in range(runs.own):
            @pl.when((e == i) & (step == last))
            def _():
                drain(runs, i, dense_out, outs, out_sem, "start")

        @pl.when((e == runs.own - 1) & (step == last))
        def _():
            for i in range(runs.own):
                drain(runs, i, dense_out, outs, out_sem, "wait")
    return after


def each_tile(tiles, work):
    big = tiles >= 4

    @pl.when(big)
    def _():
        work(0, 4 * TILE)

    lax.fori_loop(jnp.where(big, 4, 0), tiles, lambda i, _: (work(i, TILE), 0)[1], 0)


def accumulate(step, last, acc, at, part, store):
    total = jnp.where(step == 0, jnp.zeros_like(part), acc[at]) + part
    acc[at] = total

    @pl.when(step == last)
    def _():
        store(total.astype(BF16))


def ffn_kernel(group, backward, table_ref, *refs):
    ins, refs = Parts(refs[:group], refs[group], table_ref[6, 0]), refs[group + 1:]
    if backward:
        h_ref, refs = refs[0], refs[1:]
    win_ref, wout_ref = refs[:2]
    outs, refs = Parts(refs[2:2 + group], refs[2 + group], table_ref[6, 0]), refs[3 + group:]
    mid_ref, clean_ref, acc, dense_in, dense_out, in_sem, out_sem = refs
    own = dense_in.shape[0]
    runs = Runs(table_ref, group, own)
    e, step, last = pl.program_id(0), pl.program_id(1), pl.num_programs(1) - 1
    dim = win_ref.shape[1]
    after = ffn_frame(runs, ins, outs, dense_in, dense_out, in_sem, out_sem)
    rows = runs.rows(e)

    def work(tile, size):
        at = pl.ds(tile * TILE if isinstance(tile, int) else pl.multiple_of(tile * TILE, TILE), size)
        of = pl.ds(tile * (TILE // GRP), size // GRP)

        @pl.when(step == 0)
        def _():
            fresh = dense_in[e, of].reshape(size, dim)
            clean_ref[at] = jnp.where(tile * TILE + iota((size, dim), 0) < rows, fresh, jnp.zeros_like(fresh))

        if backward:
            full = lax.dot_general(clean_ref[at], wout_ref[0], NT, preferred_element_type=F32)
            mid = jnp.where(h_ref[at].astype(F32) > 0.0, full, 0.0).astype(BF16)
            part = lax.dot_general(mid, win_ref[0], NT, preferred_element_type=F32)
        else:
            mid = jnp.maximum(jnp.dot(clean_ref[at], win_ref[0], preferred_element_type=F32), 0.0).astype(BF16)
            part = jnp.dot(mid, wout_ref[0], preferred_element_type=F32)
        mid_ref[at] = mid

        def store(value):
            dense_out[e, of] = value.reshape(size // GRP, GRP, dim)
        accumulate(step, last, acc, at, part, store)

    each_tile(runs.tiles(e), work)
    after()


def ffn(table, parts, hidden, w_in, w_out, capacity, block=1024):
    group = len(parts) - 1
    own, dim, ff = w_in.shape
    held = group * capacity
    extra = [] if hidden is None else [hidden]
    result = pl.pallas_call(
        functools.partial(ffn_kernel, group, hidden is not None),
        out_shape=part_shapes(group, parts[0].shape[0], parts[-1].shape[1], dim) + [
            jax.ShapeDtypeStruct((own * held, ff), BF16), jax.ShapeDtypeStruct((own * held, dim), BF16)],
        grid_spec=pltpu.PrefetchScalarGridSpec(
            num_scalar_prefetch=1, grid=(own, ff // block),
            in_specs=[ANY] * (group + 1) + [pl.BlockSpec((held, block), lambda e, f, t: (e, f))] * len(extra) + [
                pl.BlockSpec((1, dim, block), lambda e, f, t: (e, 0, f)),
                pl.BlockSpec((1, block, dim), lambda e, f, t: (e, f, 0))],
            out_specs=[ANY] * (group + 1) + [pl.BlockSpec((held, block), lambda e, f, t: (e, f)),
                                       pl.BlockSpec((held, dim), lambda e, f, t: (e, 0))],
            scratch_shapes=[pltpu.VMEM((held, dim), F32),
                            pltpu.VMEM((own, held // GRP, GRP, dim), BF16), pltpu.VMEM((own, held // GRP, GRP, dim), BF16),
                            pltpu.SemaphoreType.DMA((own, group, 2)), pltpu.SemaphoreType.DMA((own, group, 2))]),
        cost_estimate=pl.CostEstimate(flops=3 * own * held * dim * ff, bytes_accessed=40 << 20, transcendentals=0),
        name="ffn_forward" if hidden is None else "ffn_backward",
    )(table, *parts, *extra, w_in, w_out)
    return result[:group + 1], result[group + 1], result[group + 2]


def ffn_weights(table, x, dy, hidden, grad_hidden, own, group, block=1024):
    dim, ff = x.shape[1], hidden.shape[1]
    rows = x.shape[0] // own

    def kernel(table_ref, *refs):
        r = Runs(table_ref, group, own)
        return weights_body(r, *refs)

    return pl.pallas_call(
        kernel,
        out_shape=(jax.ShapeDtypeStruct((own, dim, ff), F32), jax.ShapeDtypeStruct((own, ff, dim), F32)),
        grid_spec=pltpu.PrefetchScalarGridSpec(
            num_scalar_prefetch=1, grid=(own, ff // block),
            in_specs=[pl.BlockSpec((rows, dim), lambda e, f, t: (e, 0)),
                      pl.BlockSpec((rows, dim), lambda e, f, t: (e, 0)),
                      pl.BlockSpec((rows, block), lambda e, f, t: (e, f)),
                      pl.BlockSpec((rows, block), lambda e, f, t: (e, f))],
            out_specs=[pl.BlockSpec((1, dim, block), lambda e, f, t: (e, 0, f)),
                       pl.BlockSpec((1, block, dim), lambda e, f, t: (e, f, 0))]),
        cost_estimate=pl.CostEstimate(flops=3 * own * rows * dim * ff, bytes_accessed=60 << 20, transcendentals=0),
        name="ffn_weights",
    )(table, x, dy, hidden, grad_hidden)


def weights_body(runs, x_ref, dy_ref, h_ref, dh_ref, gin_ref, gout_ref):
    tiles = runs.tiles(pl.program_id(0))

    @pl.when(tiles == 0)
    def _():
        gin_ref[...] = jnp.zeros_like(gin_ref)
        gout_ref[...] = jnp.zeros_like(gout_ref)

    def work(tile, size):
        at = pl.ds(tile * TILE if isinstance(tile, int) else pl.multiple_of(tile * TILE, TILE), size)
        gin = lax.dot_general(x_ref[at], dh_ref[at], TN, preferred_element_type=F32)
        gout = lax.dot_general(h_ref[at], dy_ref[at], TN, preferred_element_type=F32)

        if isinstance(tile, int):
            gin_ref[0] = gin
            gout_ref[0] = gout
        else:
            @pl.when(tile == 0)
            def _():
                gin_ref[0] = gin
                gout_ref[0] = gout

            @pl.when(tile > 0)
            def _():
                gin_ref[0] += gin
                gout_ref[0] += gout

    each_tile(tiles, work)


def gather_parts(group, mine_ref, parts, held, sem):
    @pl.when(pl.program_id(0) == 0)
    def _():
        for act in ("start", "wait"):
            for k in range(group):
                move(parts, k, 0, mine_ref[0, k],
                     lambda before, count, k=k: held.at[pl.ds(mine_ref[1, k] + before, count)], sem.at[k], act, True)

        def blank(i, _):
            held[i] = jnp.zeros(held.shape[1:], held.dtype)
            return 0
        lax.fori_loop(mine_ref[2, 0], held.shape[0], blank, 0)


def unpick(mine_ref, info_ref, lane_at, held, out):
    rows, (groups, _, dim) = info_ref.shape[0], held.shape
    place = info_ref[:, lane_at:lane_at + 1].astype(I32)
    few = groups * 3 // 5 // 32 * 32

    def pick(count):
        size = count * GRP
        onehot = (place == iota((rows, size), 1)).astype(F32).astype(BF16)
        out[...] = jnp.dot(onehot, held[pl.ds(0, count)].reshape(size, dim), preferred_element_type=F32)

    @pl.when(mine_ref[2, 0] <= few)
    def _():
        pick(few)

    @pl.when(mine_ref[2, 0] > few)
    def _():
        pick(groups)


def combine_kernel(group, experts, total_tokens, *refs):
    mine_ref, parts, refs = refs[0], Parts(refs[1:1 + group], refs[1 + group], refs[0][3, 0]), refs[2 + group:]
    info_ref, g_ref, x_ref, count_ref, y_ref, dl_ref, gr_ref, main_ref, held, got, sem = refs
    rows = g_ref.shape[0]
    gather_parts(group, mine_ref, parts, held, sem)
    info = info_ref[...]
    unpick(mine_ref, info_ref, experts + 3, held, got)
    y_tok = got[...]
    prob, lse = info[:, :experts], info[:, experts:experts + 1]
    gate = info[:, experts + 1:experts + 2]
    chosen = (info[:, experts + 2:experts + 3].astype(I32) == iota((rows, experts), 1)).astype(F32)
    grad_out = g_ref[...].astype(F32)
    y_out = (gate * y_tok).astype(BF16)
    y_ref[...] = y_out
    frac = count_ref[5:6, :experts].astype(F32) / total_tokens
    grad_gate = jnp.sum(grad_out * y_tok, axis=1, keepdims=True)
    mix = jnp.sum(prob * frac, axis=1, keepdims=True)
    dlogits = ((grad_gate * gate) * (chosen - prob)
               + (AUX_WEIGHT * experts / total_tokens) * prob * (frac - mix)
               + (2.0 * Z_WEIGHT / total_tokens) * lse * prob)
    dl = dlogits.astype(BF16)
    dl_ref[...] = dl

    @pl.when(pl.program_id(0) == 0)
    def _():
        gr_ref[...] = jnp.zeros_like(gr_ref)
        main_ref[...] = jnp.zeros_like(main_ref)
    gr_ref[...] += lax.dot_general(dl, x_ref[...], TN, preferred_element_type=F32)
    main_ref[...] += jnp.sum((y_out.astype(F32) * grad_out).reshape(rows // 8, 8, -1), axis=0)


def combine(mine, meta, parts, info, grad_out, x, experts, total_tokens, block=512):
    tokens, dim = x.shape
    group = len(parts) - 1
    return pl.pallas_call(
        functools.partial(combine_kernel, group, experts, total_tokens), grid=(tokens // block,),
        out_shape=(jax.ShapeDtypeStruct((tokens, dim), BF16), jax.ShapeDtypeStruct((tokens, experts), BF16),
                   jax.ShapeDtypeStruct((experts, dim), F32), jax.ShapeDtypeStruct((8, dim), F32)),
        in_specs=[pl.BlockSpec(memory_space=pltpu.SMEM)] + [ANY] * (group + 1) + [pl.BlockSpec((block, 128), lambda i: (i, 0)),
                  pl.BlockSpec((block, dim), lambda i: (i, 0)), pl.BlockSpec((block, dim), lambda i: (i, 0)),
                  pl.BlockSpec((8, 128), lambda i: (0, 0))],
        out_specs=[pl.BlockSpec((block, dim), lambda i: (i, 0)), pl.BlockSpec((block, experts), lambda i: (i, 0)),
                   pl.BlockSpec((experts, dim), lambda i: (0, 0)), pl.BlockSpec((8, dim), lambda i: (0, 0))],
        scratch_shapes=[pltpu.VMEM((send_tiles(tokens, experts), GRP, dim), BF16), pltpu.VMEM((block, dim), F32),
                        pltpu.SemaphoreType.DMA((group, 2))],
        cost_estimate=pl.CostEstimate(flops=2 * tokens * tokens * dim, bytes_accessed=8 * tokens * dim, transcendentals=0),
        name="combine",
    )(mine, *parts, info, grad_out, x, meta)


def finish_kernel(group, experts, *refs):
    mine_ref, parts = refs[0], Parts(refs[1:1 + group], refs[1 + group], refs[0][3, 0])
    info_ref, dl_ref, w_ref, out_ref, held, got, sem = refs[2 + group:]
    gather_parts(group, mine_ref, parts, held, sem)
    unpick(mine_ref, info_ref, experts + 3, held, got)
    router = jnp.dot(dl_ref[...], w_ref[...], preferred_element_type=F32)
    out_ref[...] = (got[...] + router).astype(BF16)


def finish(mine, parts, info, dl, router_t, block=512):
    tokens, experts = dl.shape
    group, dim = len(parts) - 1, router_t.shape[1]
    return pl.pallas_call(
        functools.partial(finish_kernel, group, experts), grid=(tokens // block,),
        out_shape=jax.ShapeDtypeStruct((tokens, dim), BF16),
        in_specs=[pl.BlockSpec(memory_space=pltpu.SMEM)] + [ANY] * (group + 1) + [pl.BlockSpec((block, 128), lambda i: (i, 0)),
                  pl.BlockSpec((block, experts), lambda i: (i, 0)), pl.BlockSpec((experts, dim), lambda i: (0, 0))],
        out_specs=pl.BlockSpec((block, dim), lambda i: (i, 0)),
        scratch_shapes=[pltpu.VMEM((send_tiles(tokens, experts), GRP, dim), BF16), pltpu.VMEM((block, dim), F32),
                        pltpu.SemaphoreType.DMA((group, 2))],
        cost_estimate=pl.CostEstimate(flops=2 * tokens * tokens * dim, bytes_accessed=4 * tokens * dim, transcendentals=0),
        name="finish",
    )(mine, *parts, info, dl, router_t)


def solution(mesh):
    group = mesh.shape["ep"]

    def swap(parts, spills):
        mains = [parts[0]] + [lax.ppermute(parts[k], "ep", [(i, i ^ k) for i in range(group)]) for k in range(1, group)]
        return [*mains, parts[-1]]

    def sum_all(part):
        terms = lax.all_to_all(jnp.broadcast_to(part[None], (group, *part.shape)), "ep", 0, 0, tiled=True)
        return jnp.sum(terms, axis=0)

    def device_step(x_tokens, grad_out, w_router, expert_ids, w_in, w_out):
        tokens, dim = x_tokens.shape
        experts = w_router.shape[1]
        own = w_in.shape[0]
        capacity = 5 * tokens // (4 * experts)
        total_tokens = tokens * group
        most = own * capacity // GRP
        fit, spill = most, 1

        router_t = w_router.T
        send_x, tok, mine, counts = pack(expert_ids.reshape(1, tokens), x_tokens, group, experts, capacity, fit, spill)
        meta = tally(counts, send_x[0], group, own, capacity)

        def spills():
            return meta[4, 0] > fit

        recv_x = swap(send_x, spills)
        send_dy, info, sums = route(mine, tok, x_tokens, grad_out, router_t, send_x[0], group, fit, spill)
        recv_dy = swap(send_dy, spills)

        held_y, hidden, dense_x = ffn(meta, recv_x, None, w_in, w_out, capacity)
        back_y = swap(held_y, spills)
        held_dx, grad_hidden, dense_dy = ffn(meta, recv_dy, hidden, w_in, w_out, capacity)
        back_dx = swap(held_dx, spills)
        grad_w_in, grad_w_out = ffn_weights(meta, dense_x, dense_dy, hidden, grad_hidden, own, group)

        y_out, dl, grad_router_t, main_rows = combine(mine, meta, back_y, info, grad_out, x_tokens, experts, total_tokens)
        everything = sum_all(jnp.concatenate([grad_router_t, jnp.sum(main_rows, axis=0, keepdims=True), sums[:1]], axis=0))
        route_frac = meta[5:6, :experts].astype(F32) / total_tokens
        grad_router = everything[:experts].T
        main_term = jnp.sum(everything[experts])
        aux_loss = experts * jnp.sum(route_frac[0] * everything[experts + 1, :experts]) / total_tokens
        z_loss = everything[experts + 1, experts] / total_tokens
        objective = main_term + AUX_WEIGHT * aux_loss + Z_WEIGHT * z_loss
        grad_x = finish(mine, back_dx, info, dl, router_t)
        return y_out, grad_x, objective, main_term, grad_router, grad_w_in, grad_w_out

    spec_tok = P("ep", None)
    spec_exp = P("ep", None, None)
    return jax.shard_map(device_step, mesh=mesh,
                         in_specs=(spec_tok, spec_tok, P(None, None), P("ep"), spec_exp, spec_exp),
                         out_specs=(spec_tok, spec_tok, P(), P(), P(None, None), spec_exp, spec_exp),
                         check_vma=False)
```
